256 devices in a mesh: section: 4 (over x), vocab: 16 (over z, core), dp: 4 (over y).
Axes of the slice: x: 4, y: 4, z: 8, core: 2. Of those that a mesh axis runs over, the one named last changes fastest.
Arguments:
- hidden: bfloat16 [4, 1024, 3072], P('dp', ('section', 'vocab')), may hold values from -160 to 160
- head: bfloat16 [131072, 3072], P(('section', 'vocab')), may hold values from -3 to 3
- labels: int32 [4, 1024], P('dp'), may hold values from 0 to 131071
- response_mask: int32 [4, 1024], P('dp'), may hold values from 0 to 1, as said below
- seq_pair: int32 [4, 4], P('dp'), may hold values from 0 to 15, as said below
- ref_logp: float32 [16], replicated, may hold values from -12.6 to -12.4
Outputs:
- token_logprob: float32 [4, 1024], P('dp', ('section', 'vocab'))
- pair_margin: float32 [8], replicated
- loss: float32 [], replicated
The draws below stay inside these ranges and needn't reach their ends.
Inputs may be any that keep to these rules, and one draw needn't show every extreme that they name: `response_mask`: each sequence of 256 rows has more than half of its rows set. `seq_pair`: over all replicas every slot of 0 to 15 appears once; slot q belongs to pair q // 2 and is its chosen response when q is even.
All inputs are finite; a program needn't handle non-finite values.
Results may differ from the reference program's by a relative error of at most 0.0003.
Values may be sent and summed in bfloat16 or wider, within the bound.
No kernel may reach another device: no remote copies, remote signals or barrier semaphores. Data moves between devices by JAX's collectives and lax.ppermute only.
A program may use at most 64 MiB of HBM per device.

```python
import jax
import jax.numpy as jnp
from jax import lax

D = 3072
VOCAB = 131072
SEQ_DP = 4
REPLICAS = 4
GROUP_ROWS = 1024
SEQS = 16


def head_scale(indices):
    return 0.4 + 2.0 * indices.astype(jnp.float32) / VOCAB


def head_row(key, index):
    stream = jax.random.fold_in(jax.random.fold_in(key, 101), index)
    values = jnp.clip(jax.random.normal(stream, (D,), jnp.float32), -4.0, 4.0)
    return values * head_scale(index) * D ** (-0.5)


def draw_head(key, part):
    indices = jnp.arange(VOCAB, dtype=jnp.int32)
    table = jax.vmap(lambda index: head_row(key, index))(indices)
    return table.astype(jnp.bfloat16)


def draw_hidden(key, part):
    count_rows = REPLICAS * GROUP_ROWS
    values = jnp.clip(jax.random.normal(jax.random.fold_in(key, 201), (count_rows, D), jnp.float32), -6.0, 6.0)
    return values.reshape(REPLICAS, GROUP_ROWS, D).astype(jnp.bfloat16)


def draw_response_mask(key, part):
    seq_len = GROUP_ROWS // SEQ_DP
    prompt = jax.random.randint(jax.random.fold_in(key, 301), (REPLICAS, SEQ_DP, 1), seq_len // 8, seq_len // 2)
    places = jnp.arange(seq_len, dtype=jnp.int32)[None, None, :]
    return (places >= prompt).astype(jnp.int32).reshape(REPLICAS, GROUP_ROWS)


def draw_seq_pair(key, part):
    order = jax.random.permutation(jax.random.fold_in(key, 401), REPLICAS * SEQ_DP)
    return order.astype(jnp.int32).reshape(REPLICAS, SEQ_DP)


def plant(result, own_key, low, top_value):
    shape = result.shape
    place = [jax.random.randint(jax.random.fold_in(own_key, axis), (), 0, shape[axis]) for axis in range(len(shape))]
    result = result.at[tuple(place)].set(low)
    longest = shape.index(max(shape))
    place[longest] = (place[longest] + 1) % shape[longest]
    return result.at[tuple(place)].set(top_value)


def setup_inputs(seed: int = 0) -> dict:
    splits = jax.random.split(jax.random.key(seed), 7)
    return {
        "hidden": draw_hidden(jax.random.fold_in(splits[6], 71), 0),
        "head": draw_head(jax.random.fold_in(splits[6], 71), 0),
        "labels": plant(jax.random.randint(splits[2], (REPLICAS, GROUP_ROWS), 0, VOCAB), jax.random.fold_in(splits[2], 1), 0, VOCAB - 1).astype(jnp.int32),
        "response_mask": draw_response_mask(jax.random.fold_in(splits[6], 71), 0),
        "seq_pair": draw_seq_pair(jax.random.fold_in(splits[6], 71), 0),
        "ref_logp": jnp.clip(jax.random.uniform(splits[5], (SEQS,), jnp.float32, -12.6, -12.4), -12.6, -12.4),
    }


beta_scale = 5.0


def reference(hidden, head, labels, response_mask, seq_pair, ref_logp):
    def replica_logp(packed):
        states, targets = packed
        logits = lax.dot_general(states, head, (((1,), (1,)), ((), ())), preferred_element_type=jnp.float32)
        top_logit = jnp.max(logits, axis=1)
        total = jnp.sum(jnp.exp(logits - top_logit[:, None]), axis=1)
        target_logit = jnp.take_along_axis(logits, targets[:, None], axis=1)[:, 0]
        return target_logit - top_logit - jnp.log(total)

    token_logprob = lax.map(replica_logp, (hidden, labels))
    weights = response_mask.astype(jnp.float32)
    seq_len = GROUP_ROWS // SEQ_DP
    sums = jnp.sum((token_logprob * weights).reshape(REPLICAS, SEQ_DP, seq_len), axis=2)
    counts = jnp.sum(weights.reshape(REPLICAS, SEQ_DP, seq_len), axis=2)
    means = (sums / counts).reshape(SEQS)
    slot_ids = jnp.arange(SEQS, dtype=jnp.int32)
    in_pair = (seq_pair.reshape(SEQS)[:, None] == slot_ids[None, :]).astype(jnp.float32)
    policy = jnp.sum(in_pair * means[:, None], axis=0)
    pair_margin = beta_scale * ((policy[0::2] - ref_logp[0::2]) - (policy[1::2] - ref_logp[1::2]))
    loss = jnp.mean(jnp.logaddexp(0.0, -pair_margin))
    return token_logprob, pair_margin, loss
```

```python
import jax
import jax.numpy as jnp
from jax import lax
from jax.sharding import PartitionSpec as P


SEQ_DP = 4
PLANE = ("section", "vocab")
beta_scale = 5.0

NS, NZ, NC = 4, 8, 2


def place(s, z, c):
    return (s % NS) * NZ * NC + (z % NZ) * NC + c


def move(x, steps):
    pairs = [
        (place(s, z, c), place(s + steps[c][0], z + steps[c][1], c))
        for s in range(NS)
        for z in range(NZ)
        for c in range(NC)
        if steps[c] is not None
    ]
    return lax.ppermute(x, PLANE, pairs)


def swap_cores(x):
    pairs = [(p, p ^ 1) for p in range(NS * NZ * NC)]
    return lax.ppermute(x, PLANE, pairs)


XP, XM, ZP, ZM = (1, 0), (-1, 0), (0, 1), (0, -1)


def gather_quads(own, core):
    first = core == 0
    r1p = move(own, (XP, ZP))
    r1m = move(own, (XM, ZM))
    r2p = move(r1p, (XP, ZP))
    r2m = move(r1m, (None, ZM))
    q0 = jnp.concatenate([own, r1p, r1m, r2p])
    q1p = move(q0, (ZP, XP))
    q1m = move(q0, (ZM, XM))
    t3p = move(r2p, (None, ZP))
    t3m = move(r2m, (None, ZM))
    t4 = move(t3p, (None, ZP))
    g2 = jnp.concatenate([r2m, t3p, t3m, t4])
    q2p = move(jnp.where(first, q1p, g2), (ZP, XP))
    q2m = move(jnp.where(first, q1m, g2), (ZM, XM))
    q3p = move(jnp.where(first, q2p, q1p), (ZP, XP))
    q3m = move(q2m, (ZM, XM))
    half = q3p.shape[0] // 2
    q4p = move(q3p[:half], (ZP, None))
    q4m = move(q3m[half:], (ZM, None))
    q4 = jnp.where(first, jnp.concatenate([q4p, q4m]), g2)
    return [q0, q1p, q1m, q2p, q2m, q3p, q3m, q4]


ORDER = (0, -1, 1, -2)
FAR = (2, -3, 3, -4)
BLOCKS_A = [(ds, dz) for dz in (0, -1, 1, -2, 2, -3, 3, 4) for ds in ORDER]
BLOCKS_B = [
    (ds, dz)
    for ds, dzs in ((0, ORDER), (-1, ORDER), (1, ORDER), (-1, FAR), (1, FAR), (-2, ORDER), (-2, FAR), (0, FAR))
    for dz in dzs
]


def body(hidden, head, labels, response_mask, seq_pair, ref_logp):
    rows = hidden.shape[1]
    vocab_rows = head.shape[0]
    s = lax.axis_index("section")
    zc = lax.axis_index("vocab")
    z, core = zc // 2, zc % 2
    first = core == 0
    position = lax.axis_index(PLANE)
    quads = gather_quads(hidden[0], core)
    mine = jnp.concatenate(quads)
    both = jnp.concatenate([mine, swap_cores(mine)])

    lab = labels[0].reshape(NS, NZ, NC, rows)
    lab = jnp.roll(lab, (-s, -z), (0, 1))
    lab_a = jnp.stack([lab[ds % NS, dz % NZ, 0] for ds, dz in BLOCKS_A])
    lab_b = jnp.stack([lab[ds % NS, dz % NZ, 1] for ds, dz in BLOCKS_B])
    target = jnp.concatenate([jnp.where(first, lab_a, lab_b), jnp.where(first, lab_b, lab_a)]).reshape(-1)
    target = target - position * vocab_rows

    logits = lax.dot_general(both, head, (((1,), (1,)), ((), ())), preferred_element_type=jnp.float32)
    local_max = jnp.max(logits, axis=1)
    local_sum = jnp.sum(jnp.exp(logits - local_max[:, None]), axis=1)
    column = lax.broadcasted_iota(jnp.int32, logits.shape, 1)
    label_part = jnp.sum(jnp.where(column == target[:, None], logits, 0.0), axis=1)
    stats = jnp.stack([local_max, local_sum, label_part]).reshape(3, 2, 32, rows)
    stats_a = jnp.where(first, stats[:, 0], stats[:, 1])
    stats_b = jnp.where(first, stats[:, 1], stats[:, 0])
    at_a = {(ds % NS, dz % NZ): k for k, (ds, dz) in enumerate(BLOCKS_A)}
    at_b = {(ds % NS, dz % NZ): k for k, (ds, dz) in enumerate(BLOCKS_B)}
    rel = jnp.stack(
        [part[:, at[ds, dz]] for ds in range(NS) for dz in range(NZ) for part, at in ((stats_a, at_a), (stats_b, at_b))],
        axis=1,
    ).reshape(3, NS, NZ, NC, rows)
    stats = jnp.roll(rel, (s, z), (1, 2)).reshape(3, -1)

    pieces = lax.all_to_all(jnp.broadcast_to(stats, (NS * NZ * NC, *stats.shape)), PLANE, split_axis=0, concat_axis=0, tiled=True)
    whole_max = jnp.max(pieces[:, 0], axis=0)
    total = jnp.sum(pieces[:, 1] * jnp.exp(pieces[:, 0] - whole_max), axis=0)
    label_logit = jnp.sum(pieces[:, 2], axis=0)
    logprob = label_logit - whole_max - jnp.log(total)
    token_logprob = lax.dynamic_slice_in_dim(logprob, position * rows, rows)[None, :]

    seq_len = logprob.shape[0] // SEQ_DP
    slot_count = ref_logp.shape[0]
    weights = response_mask[0].astype(jnp.float32)
    counts = jnp.sum(weights.reshape(SEQ_DP, seq_len), axis=1)
    slot_ids = lax.broadcasted_iota(jnp.int32, (SEQ_DP, slot_count), 1)
    in_pair = (seq_pair[0][:, None] == slot_ids).astype(jnp.float32)
    seq_means = jnp.sum((logprob * weights).reshape(SEQ_DP, seq_len), axis=1) / counts
    part = jnp.sum(in_pair * seq_means[:, None], axis=0)
    ring = [lax.ppermute(part, "dp", [(i, (i + d) % 4) for i in range(4)]) for d in (1, 2, 3)]
    policy = part + ring[0] + ring[1] + ring[2]
    pair_margin = beta_scale * (policy[0::2] - ref_logp[0::2] - (policy[1::2] - ref_logp[1::2]))
    loss = jnp.mean(jnp.logaddexp(0.0, -pair_margin))
    return (token_logprob, pair_margin, loss)


def solution(mesh):
    placed = (
        P("dp", PLANE, None),
        P(PLANE, None),
        P("dp", None),
        P("dp", None),
        P("dp", None),
        P(),
    )
    return jax.shard_map(
        body,
        mesh=mesh,
        in_specs=placed,
        out_specs=(P("dp", PLANE), P(), P()),
        check_vma=False,
    )
```

```python
import functools

import jax
import jax.numpy as jnp
import numpy as np
from jax import lax
from jax.experimental import pallas as pl
from jax.experimental.pallas import tpu as pltpu
from jax.sharding import PartitionSpec as P


SEQ_DP = 4
PLANE = ("section", "vocab")
beta_scale = 5.0

NS, NZ, NC = 4, 8, 2
TILE = 512


def place(s, z, c):
    return (s % NS) * NZ * NC + (z % NZ) * NC + c


def move(x, steps):
    pairs = [
        (place(s, z, c), place(s + steps[c][0], z + steps[c][1], c))
        for s in range(NS)
        for z in range(NZ)
        for c in range(NC)
        if steps[c] is not None
    ]
    return lax.ppermute(x, PLANE, pairs)


def swap_cores(x):
    pairs = [(p, p ^ 1) for p in range(NS * NZ * NC)]
    return lax.ppermute(x, PLANE, pairs)


XP, XM, ZP, ZM = (1, 0), (-1, 0), (0, 1), (0, -1)

QUADS_A = (0, -1, 1, -2, 2, -3, 3, 4)
QUADS_B = ((0, -1), (-1, -1), (1, -1), (2, -1), (1, 3), (-1, 3), (2, 3), (0, 3))


def join_kernel(*refs):
    for k in range(4):
        refs[4][pl.ds(16 * k, 16), :] = refs[k][...]


VMEM = pl.BlockSpec(memory_space=pltpu.VMEM)


def held(*arrays):
    return [pltpu.with_memory_space_constraint(a, pltpu.VMEM) for a in arrays]


def join(*pieces):
    rows, width = pieces[0].shape
    return pl.pallas_call(
        join_kernel, in_specs=[VMEM] * 4, out_specs=VMEM, out_shape=pltpu.VMEM((4 * rows, width), pieces[0].dtype)
    )(*held(*pieces))


def pick_kernel(first_ref, mine_ref, theirs_ref, out_ref):
    @pl.when(first_ref[0] == 1)
    def _():
        out_ref[...] = mine_ref[...]

    @pl.when(first_ref[0] != 1)
    def _():
        out_ref[...] = theirs_ref[...]


def pick(first, on_core_0, on_core_1):
    return pl.pallas_call(
        pick_kernel,
        in_specs=[pl.BlockSpec(memory_space=pltpu.SMEM), VMEM, VMEM],
        out_specs=VMEM,
        out_shape=pltpu.VMEM(on_core_0.shape, on_core_0.dtype),
    )(first, *held(on_core_0, on_core_1))


def gather_quads(own, first):
    r1p = move(own, (XP, ZP))
    r1m = move(own, (XM, ZM))
    r2m = move(r1m, (XM, ZM))
    r2p = move(r1p, (None, ZP))
    q0 = join(r1p, own, r1m, r2m)
    q1p = move(q0, (ZP, XP))
    q1m = move(q0, (ZM, XM))
    t3p = move(r2p, (None, ZP))
    t3m = move(r2m, (None, ZM))
    t4 = move(t3p, (None, ZP))
    g2 = join(t3m, t4, t3p, r2p)
    q2p = move(q1p, (ZP, XP))
    q2m = move(pick(first, q1m, g2), (ZM, XM))
    q3p = move(pick(first, q2p, g2), (ZP, XP))
    q3m = move(q2m, (ZM, XM))
    q4 = move(q3p, (ZP, None))
    return q0, q1p, q1m, q2p, q2m, q3p, q3m, q4, g2


def stats_kernel(*refs, pieces, seeded):
    x_refs = refs[:pieces]
    target_ref, head_ref = refs[pieces : pieces + 2]
    seed_ref = refs[pieces + 2] if seeded else None
    out_ref, rows_ref = refs[-2:]
    step = pl.program_id(0)

    @pl.when(step == 0)
    def _():
        for k in range(4):
            block = x_refs[k][...]
            if k == 3 and pieces == 5:
                block = block + x_refs[4][...]
            rows_ref[pl.ds(64 * k, 64), :] = block
        if seeded:
            out_ref[...] = seed_ref[...]
        else:
            out_ref[...] = jnp.zeros_like(out_ref)
            out_ref[0:1, :] = jnp.full((1, out_ref.shape[1]), -jnp.inf, jnp.float32)

    logits = lax.dot_general(
        head_ref[...], rows_ref[...], (((1,), (1,)), ((), ())), preferred_element_type=jnp.float32
    )
    old_max = out_ref[0:1, :]
    new_max = jnp.maximum(old_max, jnp.max(logits, axis=0, keepdims=True))
    index = lax.broadcasted_iota(jnp.int32, logits.shape, 0) + step * logits.shape[0]
    picked = jnp.sum(jnp.where(index == target_ref[...], logits, 0.0), axis=0, keepdims=True)
    added = jnp.sum(jnp.exp(logits - new_max), axis=0, keepdims=True)
    out_ref[1:2, :] = out_ref[1:2, :] * jnp.exp(old_max - new_max) + added
    out_ref[2:3, :] = out_ref[2:3, :] + picked
    out_ref[0:1, :] = new_max


def chunk_stats(xs, target, head, seed=None):
    vocab_rows, width = head.shape
    rows = target.shape[1]
    ins = [*held(*xs), target, pltpu.with_memory_space_constraint(head, pltpu.HBM)] + ([] if seed is None else [seed])
    whole = lambda a: pl.BlockSpec(a.shape, lambda i: (0,) * a.ndim)
    specs = [VMEM for x in xs] + [whole(target), pl.BlockSpec((TILE, width), lambda i: (i, 0))]
    if seed is not None:
        specs.append(whole(seed))
    return pl.pallas_call(
        functools.partial(stats_kernel, pieces=len(xs), seeded=seed is not None),
        grid=(vocab_rows // TILE,),
        in_specs=specs,
        out_specs=pl.BlockSpec((8, rows), lambda i: (0, 0)),
        out_shape=jax.ShapeDtypeStruct((8, rows), jnp.float32),
        scratch_shapes=[pltpu.VMEM((rows, width), jnp.bfloat16)],
        cost_estimate=pl.CostEstimate(
            flops=2 * vocab_rows * width * rows, bytes_accessed=2 * vocab_rows * width, transcendentals=vocab_rows * rows
        ),
        compiler_params=pltpu.CompilerParams(dimension_semantics=("arbitrary",), vmem_limit_bytes=32 * 1024 * 1024),
    )(*ins)


def copies(x, n):
    return jnp.broadcast_to(x, (n, *x.shape))


def combine(pieces):
    top = jnp.max(pieces[:, 0], axis=0)
    total = jnp.sum(pieces[:, 1] * jnp.exp(pieces[:, 0] - top), axis=0)
    return top, total, jnp.sum(pieces[:, 2], axis=0)


def body(hidden, head, labels, response_mask, seq_pair, ref_logp):
    rows = hidden.shape[1]
    vocab_rows = head.shape[0]
    s = lax.axis_index("section")
    zc = lax.axis_index("vocab")
    z, core = zc // NC, zc % NC
    first = core == 0
    position = lax.axis_index(PLANE)

    other_head = swap_cores(head)
    flag = jnp.reshape(1 - core, (1,))
    q0, q1p, q1m, q2p, q2m, q3p, q3m, q4, g2 = gather_quads(hidden[0], flag)

    n = np.arange(8 * 4 * rows)
    quad, block, row = n // (4 * rows), n // rows % 4, n % rows
    ds_a, dz_a = block - 1, np.asarray(QUADS_A)[quad]
    ds_b, dz_b = np.asarray(QUADS_B)[quad, 0], block + np.asarray(QUADS_B)[quad, 1]
    to_s = (s + jnp.where(first, ds_a, ds_b)) % NS
    to_z = (z + jnp.where(first, dz_a, dz_b)) % NZ
    to = (to_s * NZ + to_z) * rows + row
    mine = lambda a: jnp.where(first, a[:, 0], a[:, 1]).reshape(-1)
    lab = mine(labels[0].reshape(NS * NZ, NC, rows))
    hit = n[:, None] == to[None, :]
    target = jnp.sum(jnp.where(hit, lab[:, None], 0), axis=0).reshape(2, 1, 4 * 4 * rows)
    own_target = target - position * vocab_rows
    other_target = target - (position ^ 1) * vocab_rows

    early = (q0, q1p, q1m, q2p)
    late = (q2m, q3p, q3m, q4, g2)
    stats1 = chunk_stats(early, own_target[0], head)
    stats1 = chunk_stats(early, other_target[0], other_head, stats1)
    stats2 = chunk_stats(late, own_target[1], head)
    stats2 = chunk_stats(late, other_target[1], other_head, stats2)

    stats = jnp.concatenate([stats1, stats2], axis=1)
    stats = lax.dot_general(
        stats, hit.astype(jnp.float32), (((1,), (1,)), ((), ())), precision=lax.Precision.HIGHEST
    )[:3]

    pieces = lax.all_to_all(copies(stats, NS), "section", split_axis=0, concat_axis=0, tiled=True)
    stats = jnp.stack(combine(pieces))
    along_z = [[NC * k + c for k in range(NZ)] for c in range(NC)]
    pieces = lax.all_to_all(copies(stats, NZ), "vocab", split_axis=0, concat_axis=0, tiled=True, axis_index_groups=along_z)
    top, total, label_logit = combine(pieces)
    logprob = label_logit - top - jnp.log(total)
    token_logprob = lax.dynamic_slice_in_dim(logprob, (s * NZ + z) * rows, rows)[None, :]

    slot_count = ref_logp.shape[0]
    weights = response_mask[0].astype(jnp.float32).reshape(NS, NZ * NC * rows)
    weights = weights / jnp.sum(weights, axis=1, keepdims=True)
    weights = mine(weights.reshape(NS * NZ, NC, rows))
    slots = jnp.broadcast_to(seq_pair[0][:, None], (NS, NZ * rows)).reshape(-1)
    slot_ids = lax.broadcasted_iota(jnp.int32, (slot_count, slots.shape[0]), 0)
    by_slot = jnp.where(slots[None, :] == slot_ids, weights[None, :], 0.0)
    part = jnp.sum(by_slot * logprob[None, :], axis=1)
    chips = [[(NC * k + c) * 4 + d for c in range(NC) for d in range(4)] for k in range(NZ)]
    parts = lax.all_to_all(copies(part, NC * 4), ("vocab", "dp"), split_axis=0, concat_axis=0, tiled=True, axis_index_groups=chips)
    policy = jnp.sum(parts, axis=0)
    pair_margin = beta_scale * (policy[0::2] - ref_logp[0::2] - (policy[1::2] - ref_logp[1::2]))
    loss = jnp.mean(jnp.logaddexp(0.0, -pair_margin))
    return (token_logprob, pair_margin, loss)


def solution(mesh):
    placed = (
        P("dp", PLANE, None),
        P(PLANE, None),
        P("dp", None),
        P("dp", None),
        P("dp", None),
        P(),
    )
    return jax.shard_map(
        body,
        mesh=mesh,
        in_specs=placed,
        out_specs=(P("dp", PLANE), P(), P()),
        check_vma=False,
    )
```

```python
import functools

import jax
import jax.numpy as jnp
import numpy as np
from jax import lax
from jax.experimental import pallas as pl
from jax.experimental.pallas import tpu as pltpu
from jax.sharding import PartitionSpec as P


PLANE = ("section", "vocab")
beta_scale = 5.0

NS, NZ, NC = 4, 8, 2
TILE = 512


def place(s, z, c):
    return (s % NS) * NZ * NC + (z % NZ) * NC + c


def move(x, steps):
    pairs = [
        (place(s, z, c), place(s + steps[c][0], z + steps[c][1], c))
        for s in range(NS)
        for z in range(NZ)
        for c in range(NC)
        if steps[c] is not None
    ]
    return lax.ppermute(x, PLANE, pairs)


def swap_cores(x):
    pairs = [(p, p ^ 1) for p in range(NS * NZ * NC)]
    return lax.ppermute(x, PLANE, pairs)


XP, XM, ZP, ZM = (1, 0), (-1, 0), (0, 1), (0, -1)

QUADS_A = (0, -1, 1, -2, 2, -3, 3, 4)
QUADS_B = ((0, -1), (-1, -1), (1, -1), (2, -1), (1, 3), (-1, 3), (2, 3), (0, 3))


def join_kernel(*refs):
    for k in range(4):
        refs[4][pl.ds(16 * k, 16), :] = refs[k][...]


VMEM = pl.BlockSpec(memory_space=pltpu.VMEM)
SMALL = pltpu.CompilerParams(vmem_limit_bytes=4 * 1024 * 1024)


def held(*arrays):
    return [pltpu.with_memory_space_constraint(a, pltpu.VMEM) for a in arrays]


def join(*pieces):
    rows, width = pieces[0].shape
    return pl.pallas_call(
        join_kernel, in_specs=[VMEM] * 4, out_specs=VMEM, out_shape=pltpu.VMEM((4 * rows, width), pieces[0].dtype),
        compiler_params=SMALL,
    )(*held(*pieces))


def pick_kernel(first_ref, mine_ref, theirs_ref, out_ref):
    @pl.when(first_ref[0] == 1)
    def _():
        out_ref[...] = mine_ref[...]

    @pl.when(first_ref[0] != 1)
    def _():
        out_ref[...] = theirs_ref[...]


def pick(first, on_core_0, on_core_1):
    return pl.pallas_call(
        pick_kernel,
        in_specs=[pl.BlockSpec(memory_space=pltpu.SMEM), VMEM, VMEM],
        out_specs=VMEM,
        out_shape=pltpu.VMEM(on_core_0.shape, on_core_0.dtype),
        compiler_params=SMALL,
    )(first, *held(on_core_0, on_core_1))


def copy_kernel(in_ref, out_ref):
    out_ref[...] = in_ref[...]


def gather_quads(own, first, *small):
    kept = pl.pallas_call(
        copy_kernel, in_specs=[VMEM], out_specs=VMEM, out_shape=pltpu.VMEM(own.shape, own.dtype), compiler_params=SMALL
    )(own)
    r1p = move(own, (XP, ZP))
    r1m = move(own, (XM, ZM))
    r2m = move(r1m, (XM, ZM))
    r2p = move(r1p, (None, ZP))
    q0 = join(r1p, kept, r1m, r2m)
    q1p = move(q0, (ZP, XP))
    q1m = move(q0, (ZM, XM))
    q1p, *small = lax.optimization_barrier((q1p, *small))
    t3p = move(r2p, (None, ZP))
    t3m = move(r2m, (None, ZM))
    t4 = move(r2m, (None, (0, -2)))
    g2 = join(t3m, t4, t3p, r2p)
    q2p = move(q1p, (ZP, XP))
    q2m = move(pick(first, q1m, g2), (ZM, XM))
    q3p = move(pick(first, q2p, g2), (ZP, XP))
    q3m = move(q2m, (ZM, XM))
    q4 = move(q3p, (ZP, None))
    return (q0, q1p, q1m, q2p, q2m, q3p, q3m, q4, g2), small


def stats_kernel(*refs, pieces, heads, seeded):
    x_refs = refs[:pieces]
    target_ref = refs[pieces]
    head_refs = refs[pieces + 1 : pieces + 1 + heads]
    seed_ref = refs[pieces + 1 + heads] if seeded else None
    out_ref, rows_ref, tiles_ref, arrived = refs[-4:]
    step = pl.program_id(0)
    per_head = head_refs[0].shape[0] // TILE
    steps = heads * per_head
    slots = tiles_ref.shape[0]

    def fetch(k):
        slot = lax.rem(k, slots)
        for h in range(heads):

            @pl.when(k // per_head == h)
            def _():
                tile = head_refs[h].at[pl.ds((k - h * per_head) * TILE, TILE), :]
                pltpu.make_async_copy(tile, tiles_ref.at[slot], arrived.at[slot]).start()

    @pl.when(step == 0)
    def _():
        for k in range(slots - 1):
            fetch(k)
        for k in range(4):
            block = x_refs[k][...]
            if k == 3 and pieces == 5:
                block = block + x_refs[4][...]
            rows_ref[pl.ds(64 * k, 64), :] = block
        if seeded:
            out_ref[...] = seed_ref[...]
        else:
            out_ref[...] = jnp.zeros_like(out_ref)
            out_ref[0:1, :] = jnp.full((1, out_ref.shape[1]), -jnp.inf, jnp.float32)

    @pl.when(step + slots - 1 < steps)
    def _():
        fetch(step + slots - 1)

    slot = lax.rem(step, slots)
    pltpu.make_async_copy(tiles_ref.at[slot], tiles_ref.at[slot], arrived.at[slot]).wait()
    logits = lax.dot_general(
        tiles_ref[slot], rows_ref[...], (((1,), (1,)), ((), ())), preferred_element_type=jnp.float32
    )
    which = step // per_head
    target = target_ref[0:1, :] if heads == 1 else jnp.where(which == 0, target_ref[0:1, :], target_ref[1:2, :])
    old_max = out_ref[0:1, :]
    new_max = jnp.maximum(old_max, jnp.max(logits, axis=0, keepdims=True))
    index = lax.broadcasted_iota(jnp.int32, logits.shape, 0)
    hit = index == target - (step - which * per_head) * TILE
    picked = jnp.sum(jnp.where(hit, logits, 0.0), axis=0, keepdims=True)
    added = jnp.sum(jnp.exp(logits - new_max), axis=0, keepdims=True)
    out_ref[1:2, :] = out_ref[1:2, :] * jnp.exp(old_max - new_max) + added
    out_ref[2:3, :] = out_ref[2:3, :] + picked
    out_ref[0:1, :] = new_max


def chunk_stats(xs, targets, heads, seed=None):
    vocab_rows, width = heads[0].shape
    rows = targets.shape[1]
    ins = [*held(*xs), targets, *(pltpu.with_memory_space_constraint(h, pltpu.HBM) for h in heads)]
    whole = lambda a: pl.BlockSpec(a.shape, lambda i: (0,) * a.ndim)
    specs = [VMEM for x in xs] + [whole(targets)] + [pl.BlockSpec(memory_space=pltpu.HBM) for h in heads]
    if seed is not None:
        ins.append(seed)
        specs.append(whole(seed))
    work = len(heads) * vocab_rows
    return pl.pallas_call(
        functools.partial(stats_kernel, pieces=len(xs), heads=len(heads), seeded=seed is not None),
        grid=(work // TILE,),
        in_specs=specs,
        out_specs=pl.BlockSpec((8, rows), lambda i: (0, 0)),
        out_shape=jax.ShapeDtypeStruct((8, rows), jnp.float32),
        scratch_shapes=[
            pltpu.VMEM((rows, width), jnp.bfloat16),
            pltpu.VMEM((3, TILE, width), jnp.bfloat16),
            pltpu.SemaphoreType.DMA((3,)),
        ],
        cost_estimate=pl.CostEstimate(
            flops=2 * work * width * rows, bytes_accessed=2 * work * width, transcendentals=work * rows
        ),
        compiler_params=pltpu.CompilerParams(dimension_semantics=("arbitrary",), vmem_limit_bytes=32 * 1024 * 1024),
    )(*ins)


def copies(x, n):
    return jnp.broadcast_to(x, (n, *x.shape))


def combine(pieces):
    top = jnp.max(pieces[:, 0], axis=0)
    total = jnp.sum(pieces[:, 1] * jnp.exp(pieces[:, 0] - top), axis=0)
    return top, total, jnp.sum(pieces[:, 2], axis=0)


def step(hidden, head, labels, response_mask, seq_pair, ref_logp):
    rows = hidden.shape[1]
    vocab_rows = head.shape[0]
    s = lax.axis_index("section")
    zc = lax.axis_index("vocab")
    z, core = zc // NC, zc % NC
    first = core == 0
    position = lax.axis_index(PLANE)

    other_head = swap_cores(head)
    flag = jnp.reshape(1 - core, (1,))
    quads, (labels, response_mask, seq_pair) = gather_quads(hidden[0], flag, labels, response_mask, seq_pair)
    q0, q1p, q1m, q2p, q2m, q3p, q3m, q4, g2 = quads

    n = np.arange(8 * 4 * rows)
    quad, block, row = n // (4 * rows), n // rows % 4, n % rows
    ds_a, dz_a = block - 1, np.asarray(QUADS_A)[quad]
    ds_b, dz_b = np.asarray(QUADS_B)[quad, 0], block + np.asarray(QUADS_B)[quad, 1]
    to_s = (s + jnp.where(first, ds_a, ds_b)) % NS
    to_z = (z + jnp.where(first, dz_a, dz_b)) % NZ
    to = (to_s * NZ + to_z) * rows + row
    mine = lambda a: jnp.where(first, a[:, 0], a[:, 1]).reshape(-1)
    lab = mine(labels[0].reshape(NS * NZ, NC, rows))
    hit = n[:, None] == to[None, :]
    target = jnp.sum(jnp.where(hit, lab[:, None], 0), axis=0).reshape(2, 1, 4 * 4 * rows)
    target = target - jnp.stack([position, position ^ 1])[None, :, None] * vocab_rows

    early = (q0, q1p, q1m, q2p)
    late = (q2m, q3p, q3m, q4, g2)
    stats1 = chunk_stats(early, target[0, :1], [head])
    stats1 = chunk_stats(early, target[0, 1:], [other_head], stats1)
    stats2 = chunk_stats(late, target[1], [head, other_head])

    stats = jnp.concatenate([stats1, stats2], axis=1)
    stats = lax.dot_general(
        stats, hit.astype(jnp.float32), (((1,), (1,)), ((), ())), precision=lax.Precision.HIGHEST
    )[:3]

    same_core = [[NC * k + c for k in range(NS * NZ)] for c in range(NC)]
    pieces = lax.all_to_all(
        copies(stats, NS * NZ), PLANE, split_axis=0, concat_axis=0, tiled=True, axis_index_groups=same_core
    )
    top, total, label_logit = combine(pieces)
    logprob = label_logit - top - jnp.log(total)
    token_logprob = lax.dynamic_slice_in_dim(logprob, (s * NZ + z) * rows, rows)[None, :]

    slot_count = ref_logp.shape[0]
    weights = response_mask[0].astype(jnp.float32).reshape(NS, NZ * NC * rows)
    weights = weights / jnp.sum(weights, axis=1, keepdims=True)
    weights = mine(weights.reshape(NS * NZ, NC, rows))
    slots = jnp.broadcast_to(seq_pair[0][:, None], (NS, NZ * rows)).reshape(-1)
    slot_ids = lax.broadcasted_iota(jnp.int32, (slot_count, slots.shape[0]), 0)
    by_slot = jnp.where(slots[None, :] == slot_ids, weights[None, :], 0.0)
    part = jnp.sum(by_slot * logprob[None, :], axis=1)
    part = part + swap_cores(part)
    around = [lax.ppermute(part, "dp", [(i, (i + d) % 4) for i in range(4)]) for d in (1, 3, 2)]
    policy = part + around[0] + around[1] + around[2]
    pair_margin = beta_scale * (policy[0::2] - ref_logp[0::2] - (policy[1::2] - ref_logp[1::2]))
    loss = jnp.mean(jnp.logaddexp(0.0, -pair_margin))
    return (token_logprob, pair_margin, loss)


def solution(mesh):
    placed = (
        P("dp", PLANE, None),
        P(PLANE, None),
        P("dp", None),
        P("dp", None),
        P("dp", None),
        P(),
    )
    return jax.shard_map(
        step,
        mesh=mesh,
        in_specs=placed,
        out_specs=(P("dp", PLANE), P(), P()),
        check_vma=False,
    )
```

```python
import functools

import jax
import jax.numpy as jnp
import numpy as np
from jax import lax
from jax.experimental import pallas as pl
from jax.experimental.pallas import tpu as pltpu
from jax.sharding import PartitionSpec as P


PLANE = ("section", "vocab")
beta_scale = 5.0

NS, NZ, NC = 4, 8, 2
TILE = 512


def place(s, z, c):
    return (s % NS) * NZ * NC + (z % NZ) * NC + c


def move(x, steps):
    pairs = [
        (place(s, z, c), place(s + steps[c][0], z + steps[c][1], c))
        for s in range(NS)
        for z in range(NZ)
        for c in range(NC)
        if steps[c] is not None
    ]
    return lax.ppermute(x, PLANE, pairs)


def swap_cores(x):
    pairs = [(p, p ^ 1) for p in range(NS * NZ * NC)]
    return lax.ppermute(x, PLANE, pairs)


XP, XM, ZP, ZM = (1, 0), (-1, 0), (0, 1), (0, -1)

QUADS_A = (0, -1, 1, -2, -3, 3, 4, 2)
QUADS_B = ((0, -1), (-1, -1), (1, -1), (2, -1), (-1, 3), (1, 3), (2, 3), (0, 3))


def join_kernel(*refs):
    k, rows = len(refs) - 1, refs[0].shape[0]
    for i in range(k):
        refs[k][pl.ds(rows * i, rows), :] = refs[i][...]


VMEM = pl.BlockSpec(memory_space=pltpu.VMEM)
SMALL = pltpu.CompilerParams(vmem_limit_bytes=4 * 1024 * 1024)


def held(*arrays):
    return [pltpu.with_memory_space_constraint(a, pltpu.VMEM) for a in arrays]


def join(*pieces):
    rows, width = pieces[0].shape
    return pl.pallas_call(
        join_kernel,
        in_specs=[VMEM] * len(pieces),
        out_specs=VMEM,
        out_shape=pltpu.VMEM((len(pieces) * rows, width), pieces[0].dtype),
        compiler_params=SMALL,
    )(*held(*pieces))


def pick_kernel(first_ref, mine_ref, theirs_ref, out_ref):
    @pl.when(first_ref[0] == 1)
    def _():
        out_ref[...] = mine_ref[...]

    @pl.when(first_ref[0] != 1)
    def _():
        out_ref[...] = theirs_ref[...]


def pick(first, on_core_0, on_core_1):
    return pl.pallas_call(
        pick_kernel,
        in_specs=[pl.BlockSpec(memory_space=pltpu.SMEM), VMEM, VMEM],
        out_specs=VMEM,
        out_shape=pltpu.VMEM(on_core_0.shape, on_core_0.dtype),
        compiler_params=SMALL,
    )(first, *held(on_core_0, on_core_1))


def copy_kernel(in_ref, out_ref):
    out_ref[...] = in_ref[...]


def gather_quads(own, first, *small):
    kept = pl.pallas_call(
        copy_kernel, in_specs=[VMEM], out_specs=VMEM, out_shape=pltpu.VMEM(own.shape, own.dtype), compiler_params=SMALL
    )(own)
    r1p = move(own, (XP, ZP))
    r1m = move(own, (XM, ZM))
    r2m = move(r1m, (XM, ZM))
    behind, ahead = join(r1p, kept), join(r1m, r2m)
    q0 = join(behind, ahead)
    q1p = move(q0, (ZP, XP))
    q1m = move(q0, (ZM, XM))
    f3 = move(ahead, (None, (0, -2)))
    f5 = move(behind, (None, (0, 2)))
    q1p, *small = lax.optimization_barrier((q1p, *small))
    q2p = move(q1p, (ZP, XP))
    q2m = move(q1m, (ZM, None))
    far = join(f3, f5)
    q3p = move(pick(first, q2p, far), (ZP, XP))
    q3m = move(pick(first, q2m, far), (ZM, XM))
    q4 = move(q3p, (ZP, XP))
    return (q0, q1p, q1m, q2p, q3p, q3m, q4, q2m, far), small


def stats_kernel(*refs, pieces, heads, seeded):
    x_refs = refs[:pieces]
    target_ref = refs[pieces]
    head_refs = refs[pieces + 1 : pieces + 1 + heads]
    seed_ref = refs[pieces + 1 + heads] if seeded else None
    out_ref, rows_ref, tiles_ref, arrived = refs[-4:]
    step = pl.program_id(0)
    per_head = head_refs[0].shape[0] // TILE
    steps = heads * per_head
    slots = tiles_ref.shape[0]

    def fetch(k):
        slot = lax.rem(k, slots)
        for h in range(heads):

            @pl.when(k // per_head == h)
            def _():
                tile = head_refs[h].at[pl.ds((k - h * per_head) * TILE, TILE), :]
                pltpu.make_async_copy(tile, tiles_ref.at[slot], arrived.at[slot]).start()

    @pl.when(step == 0)
    def _():
        for k in range(slots - 1):
            fetch(k)
        for k in range(4):
            block = x_refs[k][...]
            if k == 3 and pieces == 5:
                block = block + x_refs[4][...]
            rows_ref[pl.ds(64 * k, 64), :] = block
        if seeded:
            out_ref[...] = seed_ref[...]
        else:
            out_ref[...] = jnp.zeros_like(out_ref)
            out_ref[0:1, :] = jnp.full((1, out_ref.shape[1]), -jnp.inf, jnp.float32)

    @pl.when(step + slots - 1 < steps)
    def _():
        fetch(step + slots - 1)

    slot = lax.rem(step, slots)
    pltpu.make_async_copy(tiles_ref.at[slot], tiles_ref.at[slot], arrived.at[slot]).wait()
    logits = lax.dot_general(
        tiles_ref[slot], rows_ref[...], (((1,), (1,)), ((), ())), preferred_element_type=jnp.float32
    )
    which = step // per_head
    target = target_ref[0:1, :] if heads == 1 else jnp.where(which == 0, target_ref[0:1, :], target_ref[1:2, :])
    old_max = out_ref[0:1, :]
    new_max = jnp.maximum(old_max, jnp.max(logits, axis=0, keepdims=True))
    index = lax.broadcasted_iota(jnp.int32, logits.shape, 0)
    hit = index == target - (step - which * per_head) * TILE
    picked = jnp.sum(jnp.where(hit, logits, 0.0), axis=0, keepdims=True)
    added = jnp.sum(jnp.exp(logits - new_max), axis=0, keepdims=True)
    out_ref[1:2, :] = out_ref[1:2, :] * jnp.exp(old_max - new_max) + added
    out_ref[2:3, :] = out_ref[2:3, :] + picked
    out_ref[0:1, :] = new_max


def chunk_stats(xs, targets, heads, seed=None):
    vocab_rows, width = heads[0].shape
    rows = targets.shape[1]
    ins = [*held(*xs), targets, *(pltpu.with_memory_space_constraint(h, pltpu.HBM) for h in heads)]
    whole = lambda a: pl.BlockSpec(a.shape, lambda i: (0,) * a.ndim)
    specs = [VMEM for x in xs] + [whole(targets)] + [pl.BlockSpec(memory_space=pltpu.HBM) for h in heads]
    if seed is not None:
        ins.append(seed)
        specs.append(whole(seed))
    work = len(heads) * vocab_rows
    return pl.pallas_call(
        functools.partial(stats_kernel, pieces=len(xs), heads=len(heads), seeded=seed is not None),
        grid=(work // TILE,),
        in_specs=specs,
        out_specs=pl.BlockSpec((8, rows), lambda i: (0, 0)),
        out_shape=jax.ShapeDtypeStruct((8, rows), jnp.float32),
        scratch_shapes=[
            pltpu.VMEM((rows, width), jnp.bfloat16),
            pltpu.VMEM((3, TILE, width), jnp.bfloat16),
            pltpu.SemaphoreType.DMA((3,)),
        ],
        cost_estimate=pl.CostEstimate(
            flops=2 * work * width * rows, bytes_accessed=2 * work * width, transcendentals=work * rows
        ),
        compiler_params=pltpu.CompilerParams(dimension_semantics=("arbitrary",), vmem_limit_bytes=32 * 1024 * 1024),
    )(*ins)


def copies(x, n):
    return jnp.broadcast_to(x, (n, *x.shape))


def combine(pieces):
    top = jnp.max(pieces[:, 0], axis=0)
    total = jnp.sum(pieces[:, 1] * jnp.exp(pieces[:, 0] - top), axis=0)
    return top, total, jnp.sum(pieces[:, 2], axis=0)


def step(hidden, head, labels, response_mask, seq_pair, ref_logp):
    rows = hidden.shape[1]
    vocab_rows = head.shape[0]
    s = lax.axis_index("section")
    zc = lax.axis_index("vocab")
    z, core = zc // NC, zc % NC
    first = core == 0
    position = lax.axis_index(PLANE)

    other_head = swap_cores(head)
    flag = jnp.reshape(1 - core, (1,))
    quads, (labels, s, z, core) = gather_quads(hidden[0], flag, labels, s, z, core)
    first = core == 0
    early, late = quads[:4], quads[4:]

    n = np.arange(8 * 4 * rows)
    quad, block, row = n // (4 * rows), n // rows % 4, n % rows
    ds_a, dz_a = block - 1, np.asarray(QUADS_A)[quad]
    ds_b, dz_b = np.asarray(QUADS_B)[quad, 0], block + np.asarray(QUADS_B)[quad, 1]
    to_s = (s + jnp.where(first, ds_a, ds_b)) % NS
    to_z = (z + jnp.where(first, dz_a, dz_b)) % NZ
    to = (to_s * NZ + to_z) * rows + row
    mine = lambda a: jnp.where(first, a[:, 0], a[:, 1]).reshape(-1)
    lab = mine(labels[0].reshape(NS * NZ, NC, rows))
    hit = n[:, None] == to[None, :]
    target = jnp.sum(jnp.where(hit, lab[:, None], 0), axis=0).reshape(2, 1, 4 * 4 * rows)
    target = target - jnp.stack([position, position ^ 1])[None, :, None] * vocab_rows

    stats1 = chunk_stats(early, target[0, :1], [head])
    stats1 = chunk_stats(early, target[0, 1:], [other_head], stats1)
    stats2 = chunk_stats(late, target[1], [head, other_head])

    stats = jnp.concatenate([stats1, stats2], axis=1)
    stats = lax.dot_general(
        stats, hit.astype(jnp.float32), (((1,), (1,)), ((), ())), precision=lax.Precision.HIGHEST
    )[:3]

    same_core = [[NC * k + c for k in range(NS * NZ)] for c in range(NC)]
    stats, response_mask, seq_pair, ref_logp = lax.optimization_barrier((stats, response_mask, seq_pair, ref_logp))
    sent = copies(stats, NS * NZ)
    pieces = lax.all_to_all(sent, PLANE, split_axis=0, concat_axis=0, tiled=True, axis_index_groups=same_core)
    top, total, label_logit = combine(pieces)
    logprob = label_logit - top - jnp.log(total)
    token_logprob = lax.dynamic_slice_in_dim(logprob, (s * NZ + z) * rows, rows)[None, :]

    slot_count = ref_logp.shape[0]
    weights = response_mask[0].astype(jnp.float32).reshape(NS, NZ * NC * rows)
    weights = weights / jnp.sum(weights, axis=1, keepdims=True)
    weights = mine(weights.reshape(NS * NZ, NC, rows))
    slots = jnp.broadcast_to(seq_pair[0][:, None], (NS, NZ * rows)).reshape(-1)
    slot_ids = lax.broadcasted_iota(jnp.int32, (slot_count, slots.shape[0]), 0)
    by_slot = jnp.where(slots[None, :] == slot_ids, weights[None, :], 0.0)
    part = jnp.sum(by_slot * logprob[None, :], axis=1)
    part = part + swap_cores(part)
    around = [lax.ppermute(part, "dp", [(i, (i + d) % 4) for i in range(4)]) for d in (1, 3, 2)]
    policy = part + around[0] + around[1] + around[2]
    pair_margin = beta_scale * (policy[0::2] - ref_logp[0::2] - (policy[1::2] - ref_logp[1::2]))
    loss = jnp.mean(jnp.logaddexp(0.0, -pair_margin))
    return (token_logprob, pair_margin, loss)


def solution(mesh):
    placed = (
        P("dp", PLANE, None),
        P(PLANE, None),
        P("dp", None),
        P("dp", None),
        P("dp", None),
        P(),
    )
    return jax.shard_map(
        step,
        mesh=mesh,
        in_specs=placed,
        out_specs=(P("dp", PLANE), P(), P()),
        check_vma=False,
    )
```

```python
import functools

import jax
import jax.numpy as jnp
import numpy as np
from jax import lax
from jax.experimental import pallas as pl
from jax.experimental.pallas import tpu as pltpu
from jax.sharding import PartitionSpec as P


PLANE = ("section", "vocab")
beta_scale = 5.0

NS, NZ, NC = 4, 8, 2
TILE = 512


def place(s, z, c):
    return (s % NS) * NZ * NC + (z % NZ) * NC + c


def move(x, steps):
    pairs = [
        (place(s, z, c), place(s + steps[c][0], z + steps[c][1], c))
        for s in range(NS)
        for z in range(NZ)
        for c in range(NC)
        if steps[c] is not None
    ]
    return lax.ppermute(x, PLANE, pairs)


def swap_cores(x):
    pairs = [(p, p ^ 1) for p in range(NS * NZ * NC)]
    return lax.ppermute(x, PLANE, pairs)


XP, XM, ZP, ZM = (1, 0), (-1, 0), (0, 1), (0, -1)

QUADS_A = (0, -1, 1, -2, -3, 3, 4, 2)
QUADS_B = ((0, -1), (-1, -1), (1, -1), (2, -1), (-1, 3), (1, 3), (2, 3), (0, 3))


def join_kernel(*refs):
    k, rows = len(refs) - 1, refs[0].shape[0]
    for i in range(k):
        refs[k][pl.ds(rows * i, rows), :] = refs[i][...]


VMEM = pl.BlockSpec(memory_space=pltpu.VMEM)
SMALL = pltpu.CompilerParams(vmem_limit_bytes=4 * 1024 * 1024)


def held(*arrays):
    return [pltpu.with_memory_space_constraint(a, pltpu.VMEM) for a in arrays]


def join(*pieces):
    rows, width = pieces[0].shape
    return pl.pallas_call(
        join_kernel,
        in_specs=[VMEM] * len(pieces),
        out_specs=VMEM,
        out_shape=pltpu.VMEM((len(pieces) * rows, width), pieces[0].dtype),
        compiler_params=SMALL,
    )(*held(*pieces))


def pick_kernel(first_ref, mine_ref, theirs_ref, out_ref):
    @pl.when(first_ref[0] == 1)
    def _():
        out_ref[...] = mine_ref[...]

    @pl.when(first_ref[0] != 1)
    def _():
        out_ref[...] = theirs_ref[...]


def pick(first, on_core_0, on_core_1):
    return pl.pallas_call(
        pick_kernel,
        in_specs=[pl.BlockSpec(memory_space=pltpu.SMEM), VMEM, VMEM],
        out_specs=VMEM,
        out_shape=pltpu.VMEM(on_core_0.shape, on_core_0.dtype),
        compiler_params=SMALL,
    )(first, *held(on_core_0, on_core_1))


def copy_kernel(in_ref, out_ref):
    out_ref[...] = in_ref[...]


def gather_quads(own, first):
    kept = pl.pallas_call(
        copy_kernel, in_specs=[VMEM], out_specs=VMEM, out_shape=pltpu.VMEM(own.shape, own.dtype), compiler_params=SMALL
    )(own)
    r1p = move(own, (XP, ZP))
    r1m = move(own, (XM, ZM))
    r2m = move(r1m, (XM, ZM))
    behind, ahead = join(r1p, kept), join(r1m, r2m)
    q0 = join(behind, ahead)
    q1p = move(q0, (ZP, XP))
    q1m = move(q0, (ZM, XM))
    f3 = move(ahead, (None, (0, -2)))
    f5 = move(behind, (None, (0, 2)))
    q2p = move(q1p, (ZP, XP))
    q2m = move(q1m, (ZM, None))
    far = join(f3, f5)
    q3p = move(pick(first, q2p, far), (ZP, XP))
    q3m = move(pick(first, q2m, far), (ZM, XM))
    q4 = move(q3p, (ZP, XP))
    return q0, q1p, q1m, q2p, q3p, q3m, q4, q2m, far


def stats_kernel(*refs, pieces, heads, seeded, chunk, first_head):
    x_refs = refs[:pieces]
    target_ref = refs[pieces]
    head_refs = refs[pieces + 1 : pieces + 1 + heads]
    seed_ref = refs[pieces + 1 + heads] if seeded else None
    out_ref, rows_ref, tiles_ref, arrived = refs[-4:]
    step = pl.program_id(0)
    per_head = head_refs[0].shape[0] // TILE
    steps = heads * per_head
    slots = tiles_ref.shape[0]

    def fetch(k):
        slot = lax.rem(k, slots)
        for h in range(heads):

            @pl.when(k // per_head == h)
            def _():
                tile = head_refs[h].at[pl.ds((k - h * per_head) * TILE, TILE), :]
                pltpu.make_async_copy(tile, tiles_ref.at[slot], arrived.at[slot]).start()

    @pl.when(step == 0)
    def _():
        for k in range(slots - 1):
            fetch(k)
        for k in range(4):
            block = x_refs[k][...]
            if k == 3 and pieces == 5:
                block = block + x_refs[4][...]
            rows_ref[pl.ds(64 * k, 64), :] = block
        if seeded:
            out_ref[...] = seed_ref[...]
        else:
            out_ref[...] = jnp.zeros_like(out_ref)
            out_ref[0:1, :] = jnp.full((1, out_ref.shape[1]), -jnp.inf, jnp.float32)

    @pl.when(step + slots - 1 < steps)
    def _():
        fetch(step + slots - 1)

    slot = lax.rem(step, slots)
    pltpu.make_async_copy(tiles_ref.at[slot], tiles_ref.at[slot], arrived.at[slot]).wait()
    logits = lax.dot_general(
        tiles_ref[slot], rows_ref[...], (((1,), (1,)), ((), ())), preferred_element_type=jnp.float32
    )
    which = step // per_head
    target = target_ref[chunk, pl.ds(first_head + which, 1), :]
    old_max = out_ref[0:1, :]
    new_max = jnp.maximum(old_max, jnp.max(logits, axis=0, keepdims=True))
    index = lax.broadcasted_iota(jnp.int32, logits.shape, 0)
    hit = index == target - (step - which * per_head) * TILE
    picked = jnp.sum(jnp.where(hit, logits, 0.0), axis=0, keepdims=True)
    added = jnp.sum(jnp.exp(logits - new_max), axis=0, keepdims=True)
    out_ref[1:2, :] = out_ref[1:2, :] * jnp.exp(old_max - new_max) + added
    out_ref[2:3, :] = out_ref[2:3, :] + picked
    out_ref[0:1, :] = new_max


def chunk_stats(xs, targets, chunk, first_head, heads, seed=None):
    vocab_rows, width = heads[0].shape
    rows = targets.shape[2]
    ins = [*held(*xs), targets, *(pltpu.with_memory_space_constraint(h, pltpu.HBM) for h in heads)]
    whole = lambda a: pl.BlockSpec(a.shape, lambda i: (0,) * a.ndim)
    specs = [VMEM for x in xs] + [whole(targets)] + [pl.BlockSpec(memory_space=pltpu.HBM) for h in heads]
    if seed is not None:
        ins.append(seed)
        specs.append(whole(seed))
    work = len(heads) * vocab_rows
    return pl.pallas_call(
        functools.partial(
            stats_kernel,
            pieces=len(xs),
            heads=len(heads),
            seeded=seed is not None,
            chunk=chunk,
            first_head=first_head,
        ),
        grid=(work // TILE,),
        in_specs=specs,
        out_specs=pl.BlockSpec((8, rows), lambda i: (0, 0)),
        out_shape=jax.ShapeDtypeStruct((8, rows), jnp.float32),
        scratch_shapes=[
            pltpu.VMEM((rows, width), jnp.bfloat16),
            pltpu.VMEM((3, TILE, width), jnp.bfloat16),
            pltpu.SemaphoreType.DMA((3,)),
        ],
        cost_estimate=pl.CostEstimate(
            flops=2 * work * width * rows, bytes_accessed=2 * work * width, transcendentals=work * rows
        ),
        compiler_params=pltpu.CompilerParams(dimension_semantics=("arbitrary",), vmem_limit_bytes=32 * 1024 * 1024),
    )(*ins)


def copies(x, n):
    return jnp.broadcast_to(x, (n, *x.shape))


def combine(pieces):
    top = jnp.max(pieces[:, 0], axis=0)
    total = jnp.sum(pieces[:, 1] * jnp.exp(pieces[:, 0] - top), axis=0)
    return top, total, jnp.sum(pieces[:, 2], axis=0)


def step(hidden, head, labels, response_mask, seq_pair, ref_logp):
    rows = hidden.shape[1]
    vocab_rows = head.shape[0]
    s = lax.axis_index("section")
    zc = lax.axis_index("vocab")
    z, core = zc // NC, zc % NC
    first = core == 0
    position = lax.axis_index(PLANE)

    other_head = swap_cores(head)
    flag = jnp.reshape(1 - core, (1,))
    quads = gather_quads(hidden[0], flag)
    early, late = quads[:4], quads[4:]

    n = np.arange(8 * 4 * rows)
    quad, block, row = n // (4 * rows), n // rows % 4, n % rows
    ds_a, dz_a = block - 1, np.asarray(QUADS_A)[quad]
    ds_b, dz_b = np.asarray(QUADS_B)[quad, 0], block + np.asarray(QUADS_B)[quad, 1]
    to_s = (s + jnp.where(first, ds_a, ds_b)) % NS
    to_z = (z + jnp.where(first, dz_a, dz_b)) % NZ
    to = (to_s * NZ + to_z) * rows + row
    mine = lambda a: jnp.where(first, a[:, 0], a[:, 1]).reshape(-1)
    lab = mine(labels[0].reshape(NS * NZ, NC, rows))
    hit = n[:, None] == to[None, :]
    target = jnp.sum(jnp.where(hit, lab[:, None], 0), axis=0).reshape(2, 1, 4 * 4 * rows)
    target = target - jnp.stack([position, position ^ 1])[None, :, None] * vocab_rows

    stats1 = chunk_stats(early, target, 0, 0, [head])
    stats1 = chunk_stats(early, target, 0, 1, [other_head], stats1)
    stats2 = chunk_stats(late, target, 1, 0, [head, other_head])

    stats = jnp.concatenate([stats1, stats2], axis=1)
    stats = lax.dot_general(
        stats, hit.astype(jnp.float32), (((1,), (1,)), ((), ())), precision=lax.Precision.HIGHEST
    )[:3]

    same_core = [[NC * k + c for k in range(NS * NZ)] for c in range(NC)]
    sent = copies(stats, NS * NZ)
    pieces = lax.all_to_all(sent, PLANE, split_axis=0, concat_axis=0, tiled=True, axis_index_groups=same_core)
    top, total, label_logit = combine(pieces)
    logprob = label_logit - top - jnp.log(total)

    slot_count = ref_logp.shape[0]
    ref_gap = ref_logp[0::2] - ref_logp[1::2]
    own_start = (s * NZ + z) * rows
    weights = response_mask[0].astype(jnp.float32).reshape(NS, NZ * NC * rows)
    weights = weights / jnp.sum(weights, axis=1, keepdims=True)
    weights = mine(weights.reshape(NS * NZ, NC, rows))
    slots = jnp.broadcast_to(seq_pair[0][:, None], (NS, NZ * rows)).reshape(-1)
    slot_ids = lax.broadcasted_iota(jnp.int32, (slot_count, slots.shape[0]), 0)
    by_slot = jnp.where(slots[None, :] == slot_ids, weights[None, :], 0.0)
    token_logprob = lax.dynamic_slice_in_dim(logprob, own_start, rows, allow_negative_indices=False)[None, :]
    part = jnp.sum(by_slot * logprob[None, :], axis=1)
    part = part + swap_cores(part)
    around = [lax.ppermute(part, "dp", [(i, (i + d) % 4) for i in range(4)]) for d in (1, 3, 2)]
    policy = part + around[0] + around[1] + around[2]
    pair_margin = beta_scale * (policy[0::2] - policy[1::2] - ref_gap)
    loss = jnp.mean(jnp.logaddexp(0.0, -pair_margin))
    return (token_logprob, pair_margin, loss)


def solution(mesh):
    placed = (
        P("dp", PLANE, None),
        P(PLANE, None),
        P("dp", None),
        P("dp", None),
        P("dp", None),
        P(),
    )
    return jax.shard_map(
        step,
        mesh=mesh,
        in_specs=placed,
        out_specs=(P("dp", PLANE), P(), P()),
        check_vma=False,
    )
```

```python
import functools

import jax
import jax.numpy as jnp
import numpy as np
from jax import lax
from jax.experimental import pallas as pl
from jax.experimental.pallas import tpu as pltpu
from jax.sharding import PartitionSpec as P


PLANE = ("section", "vocab")
beta_scale = 5.0

NS, NZ, NC = 4, 8, 2
TILE = 512


def place(s, z, c):
    return (s % NS) * NZ * NC + (z % NZ) * NC + c


def move(x, steps):
    pairs = [
        (place(s, z, c), place(s + steps[c][0], z + steps[c][1], c))
        for s in range(NS)
        for z in range(NZ)
        for c in range(NC)
        if steps[c] is not None
    ]
    return lax.ppermute(x, PLANE, pairs)


def swap_cores(x):
    pairs = [(p, p ^ 1) for p in range(NS * NZ * NC)]
    return lax.ppermute(x, PLANE, pairs)


XP, XM, ZP, ZM = (1, 0), (-1, 0), (0, 1), (0, -1)

QUADS_A = (0, -1, 1, -2, -3, 3, 4, 2)
QUADS_B = ((0, -1), (-1, -1), (1, -1), (2, -1), (-1, 3), (1, 3), (2, 3), (0, 3))


def join_kernel(*refs):
    k, rows = len(refs) - 1, refs[0].shape[0]
    for i in range(k):
        refs[k][pl.ds(rows * i, rows), :] = refs[i][...]


VMEM = pl.BlockSpec(memory_space=pltpu.VMEM)
SMALL = pltpu.CompilerParams(vmem_limit_bytes=4 * 1024 * 1024)


def held(*arrays):
    return [pltpu.with_memory_space_constraint(a, pltpu.VMEM) for a in arrays]


def join(*pieces):
    rows, width = pieces[0].shape
    return pl.pallas_call(
        join_kernel,
        in_specs=[VMEM] * len(pieces),
        out_specs=VMEM,
        out_shape=pltpu.VMEM((len(pieces) * rows, width), pieces[0].dtype),
        compiler_params=SMALL,
    )(*held(*pieces))


def pick_kernel(first_ref, mine_ref, theirs_ref, out_ref):
    @pl.when(first_ref[0] == 1)
    def _():
        out_ref[...] = mine_ref[...]

    @pl.when(first_ref[0] != 1)
    def _():
        out_ref[...] = theirs_ref[...]


def pick(first, on_core_0, on_core_1):
    return pl.pallas_call(
        pick_kernel,
        in_specs=[pl.BlockSpec(memory_space=pltpu.SMEM), VMEM, VMEM],
        out_specs=VMEM,
        out_shape=pltpu.VMEM(on_core_0.shape, on_core_0.dtype),
        compiler_params=SMALL,
    )(first, *held(on_core_0, on_core_1))


def copy_kernel(in_ref, out_ref):
    out_ref[...] = in_ref[...]


def gather_quads(own, first):
    kept = pl.pallas_call(
        copy_kernel, in_specs=[VMEM], out_specs=VMEM, out_shape=pltpu.VMEM(own.shape, own.dtype), compiler_params=SMALL
    )(own)
    r1p = move(own, (XP, ZP))
    r1m = move(own, (XM, ZM))
    r2m = move(own, ((-2, 0), (0, -2)))
    q0 = join(r1p, kept, r1m, r2m)
    q1p = move(q0, (ZP, XP))
    q1m = move(q0, (ZM, XM))
    r2p = move(own, (None, (0, 2)))
    t3m = move(r2m, (None, ZM))
    q2p = move(q1p, (ZP, XP))
    t3p = move(r2p, (None, ZP))
    t4 = move(t3m, (None, ZM))
    q2m = move(q1m, (ZM, None))
    far = join(t3m, t4, t3p, r2p)
    q3p = move(pick(first, q2p, far), (ZP, XP))
    q3m = move(pick(first, q2m, far), (ZM, XM))
    q4 = move(q3p, (ZP, XP))
    return q0, q1p, q1m, q2p, q3p, q3m, q4, q2m, far


def stats_kernel(*refs, pieces, heads, seeded, chunk, first_head):
    x_refs = refs[:pieces]
    target_ref = refs[pieces]
    head_refs = refs[pieces + 1 : pieces + 1 + heads]
    seed_ref = refs[pieces + 1 + heads] if seeded else None
    out_ref, rows_ref, tiles_ref, arrived = refs[-4:]
    step = pl.program_id(0)
    per_head = head_refs[0].shape[0] // TILE
    steps = heads * per_head
    slots = tiles_ref.shape[0]

    def fetch(k):
        slot = lax.rem(k, slots)
        for h in range(heads):

            @pl.when(k // per_head == h)
            def _():
                tile = head_refs[h].at[pl.ds((k - h * per_head) * TILE, TILE), :]
                pltpu.make_async_copy(tile, tiles_ref.at[slot], arrived.at[slot]).start()

    @pl.when(step == 0)
    def _():
        for k in range(slots - 1):
            fetch(k)
        for k in range(4):
            block = x_refs[k][...]
            if k == 3 and pieces == 5:
                block = block + x_refs[4][...]
            rows_ref[pl.ds(64 * k, 64), :] = block
        if seeded:
            out_ref[...] = seed_ref[...]
        else:
            out_ref[...] = jnp.zeros_like(out_ref)
            out_ref[0:1, :] = jnp.full((1, out_ref.shape[1]), -jnp.inf, jnp.float32)

    @pl.when(step + slots - 1 < steps)
    def _():
        fetch(step + slots - 1)

    slot = lax.rem(step, slots)
    pltpu.make_async_copy(tiles_ref.at[slot], tiles_ref.at[slot], arrived.at[slot]).wait()
    logits = lax.dot_general(
        tiles_ref[slot], rows_ref[...], (((1,), (1,)), ((), ())), preferred_element_type=jnp.float32
    )
    which = step // per_head
    target = target_ref[chunk, pl.ds(first_head + which, 1), :]
    old_max = out_ref[0:1, :]
    new_max = jnp.maximum(old_max, jnp.max(logits, axis=0, keepdims=True))
    index = lax.broadcasted_iota(jnp.int32, logits.shape, 0)
    hit = index == target - (step - which * per_head) * TILE
    picked = jnp.sum(jnp.where(hit, logits, 0.0), axis=0, keepdims=True)
    added = jnp.sum(jnp.exp(logits - new_max), axis=0, keepdims=True)
    out_ref[1:2, :] = out_ref[1:2, :] * jnp.exp(old_max - new_max) + added
    out_ref[2:3, :] = out_ref[2:3, :] + picked
    out_ref[0:1, :] = new_max


def chunk_stats(xs, targets, chunk, first_head, heads, seed=None):
    vocab_rows, width = heads[0].shape
    rows = targets.shape[2]
    ins = [*held(*xs), targets, *(pltpu.with_memory_space_constraint(h, pltpu.HBM) for h in heads)]
    whole = lambda a: pl.BlockSpec(a.shape, lambda i: (0,) * a.ndim)
    specs = [VMEM for x in xs] + [whole(targets)] + [pl.BlockSpec(memory_space=pltpu.HBM) for h in heads]
    if seed is not None:
        ins.append(seed)
        specs.append(whole(seed))
    work = len(heads) * vocab_rows
    return pl.pallas_call(
        functools.partial(
            stats_kernel,
            pieces=len(xs),
            heads=len(heads),
            seeded=seed is not None,
            chunk=chunk,
            first_head=first_head,
        ),
        grid=(work // TILE,),
        in_specs=specs,
        out_specs=pl.BlockSpec((8, rows), lambda i: (0, 0)),
        out_shape=jax.ShapeDtypeStruct((8, rows), jnp.float32),
        scratch_shapes=[
            pltpu.VMEM((rows, width), jnp.bfloat16),
            pltpu.VMEM((3, TILE, width), jnp.bfloat16),
            pltpu.SemaphoreType.DMA((3,)),
        ],
        cost_estimate=pl.CostEstimate(
            flops=2 * work * width * rows, bytes_accessed=2 * work * width, transcendentals=work * rows
        ),
        compiler_params=pltpu.CompilerParams(dimension_semantics=("arbitrary",), vmem_limit_bytes=32 * 1024 * 1024),
    )(*ins)


def copies(x, n):
    return jnp.broadcast_to(x, (n, *x.shape))


def combine(pieces):
    top = jnp.max(pieces[:, 0], axis=0)
    total = jnp.sum(pieces[:, 1] * jnp.exp(pieces[:, 0] - top), axis=0)
    return top, total, jnp.sum(pieces[:, 2], axis=0)


def step(hidden, head, labels, response_mask, seq_pair, ref_logp):
    rows = hidden.shape[1]
    vocab_rows = head.shape[0]
    s = lax.axis_index("section")
    zc = lax.axis_index("vocab")
    z, core = zc // NC, zc % NC
    first = core == 0
    position = lax.axis_index(PLANE)

    other_head = swap_cores(head)
    flag = jnp.reshape(1 - core, (1,))
    quads = gather_quads(hidden[0], flag)
    early, late = quads[:4], quads[4:]

    n = np.arange(8 * 4 * rows)
    quad, block, row = n // (4 * rows), n // rows % 4, n % rows
    ds_a, dz_a = block - 1, np.asarray(QUADS_A)[quad]
    ds_b, dz_b = np.asarray(QUADS_B)[quad, 0], block + np.asarray(QUADS_B)[quad, 1]
    to_s = (s + jnp.where(first, ds_a, ds_b)) % NS
    to_z = (z + jnp.where(first, dz_a, dz_b)) % NZ
    to = (to_s * NZ + to_z) * rows + row
    mine = lambda a: jnp.where(first, a[:, 0], a[:, 1]).reshape(-1)
    labels = lax.optimization_barrier(labels)
    lab = mine(labels[0].reshape(NS * NZ, NC, rows))
    hit = n[:, None] == to[None, :]
    target = jnp.sum(jnp.where(hit, lab[:, None], 0), axis=0).reshape(2, 1, 4 * 4 * rows)
    target = target - jnp.stack([position, position ^ 1])[None, :, None] * vocab_rows

    stats1 = chunk_stats(early, target, 0, 0, [head])
    stats1 = chunk_stats(early, target, 0, 1, [other_head], stats1)
    stats2 = chunk_stats(late, target, 1, 0, [head, other_head])

    stats = jnp.concatenate([stats1, stats2], axis=1)
    stats = lax.dot_general(
        stats, hit.astype(jnp.float32), (((1,), (1,)), ((), ())), precision=lax.Precision.HIGHEST
    )[:3]

    same_core = [[NC * k + c for k in range(NS * NZ)] for c in range(NC)]
    sent = copies(stats, NS * NZ)
    pieces = lax.all_to_all(sent, PLANE, split_axis=0, concat_axis=0, tiled=True, axis_index_groups=same_core)
    top, total, label_logit = combine(pieces)
    logprob = label_logit - top - jnp.log(total)

    slot_count = ref_logp.shape[0]
    response_mask, ref_logp = lax.optimization_barrier((response_mask, ref_logp))
    ref_gap = ref_logp[0::2] - ref_logp[1::2]
    own_start = (s * NZ + z) * rows
    weights = response_mask[0].astype(jnp.float32).reshape(NS, NZ * NC * rows)
    weights = weights / jnp.sum(weights, axis=1, keepdims=True)
    weights = mine(weights.reshape(NS * NZ, NC, rows))
    slots = jnp.broadcast_to(seq_pair[0][:, None], (NS, NZ * rows)).reshape(-1)
    slot_ids = lax.broadcasted_iota(jnp.int32, (slot_count, slots.shape[0]), 0)
    by_slot = jnp.where(slots[None, :] == slot_ids, weights[None, :], 0.0)
    token_logprob = lax.dynamic_slice_in_dim(logprob, own_start, rows, allow_negative_indices=False)[None, :]
    part = jnp.sum(by_slot * logprob[None, :], axis=1)
    part = part + swap_cores(part)
    part = part + lax.ppermute(part, "dp", [(i, i ^ 1) for i in range(4)])
    policy = part + lax.ppermute(part, "dp", [(i, i ^ 3) for i in range(4)])
    pair_margin = beta_scale * (policy[0::2] - policy[1::2] - ref_gap)
    loss = jnp.mean(jnp.logaddexp(0.0, -pair_margin))
    return (token_logprob, pair_margin, loss)


def solution(mesh):
    placed = (
        P("dp", PLANE, None),
        P(PLANE, None),
        P("dp", None),
        P("dp", None),
        P("dp", None),
        P(),
    )
    return jax.shard_map(
        step,
        mesh=mesh,
        in_specs=placed,
        out_specs=(P("dp", PLANE), P(), P()),
        check_vma=False,
    )
```
